32 devices in a mesh: img: 8 (over y, x, core), strip: 4 (over z).
Axes of the slice: x: 2, y: 2, z: 4, core: 2. Of those that a mesh axis runs over, the one named last changes fastest.
Arguments:
- image_in: bfloat16 [8, 128, 128, 128], P('img', 'strip'), may hold values from -6 to 6
- cotangent: bfloat16 [8, 128, 128, 128], P('img', 'strip'), may hold values from -6 to 6
- conv1_w: bfloat16 [3, 3, 128, 128], replicated, may hold values from -0.1875 to 0.1875
- conv2_w: bfloat16 [3, 3, 128, 128], replicated, may hold values from -0.1875 to 0.1875
- norm1_gain: float32 [128], replicated, may hold values from 0.5 to 1.5
- norm1_shift: float32 [128], replicated, may hold values from -3 to 3
- norm2_gain: float32 [128], replicated, may hold values from 0.5 to 1.5
- norm2_shift: float32 [128], replicated, may hold values from -3 to 3
- strip_rows: int32 [8, 4], P('img', 'strip'), may hold values from 1 to 32, 64 in all within a row
Outputs:
- image_grad: bfloat16 [8, 128, 128, 128], P('img', 'strip')
- conv1_grad: float32 [1152, 128], P('img')
- conv2_grad: float32 [1152, 128], P('img')
- norm_grads: float32 [4, 128], replicated
The draws below stay inside these ranges and needn't reach their ends.
Inputs may be any that keep to these rules, and one draw needn't show every extreme that they name: `strip_rows`: each image's 4 strip lengths sum to 64; in every image one strip holds exactly 32 rows.
All inputs are finite; a program needn't handle non-finite values. No bound on the sum of `strip_rows` on one device may be relied on, other than what follows from the above.
Results may differ from the reference program's by a relative error of at most 0.0055.
Values may be sent and summed in bfloat16 or wider, within the bound.
A program may use at most 64 MiB of HBM per device.

```python
import math
import jax
import jax.numpy as jnp
import numpy as np
from jax import lax

C = 128
GROUPS = 32
CAP = 32
COLS = 128
IMAGES = 8
ROWS_ALL = 128
HEIGHT = 64
N_STRIP = 4


def steps_of(rng, extent, pieces, smallest, top_value):
    def one(dim, parts):
        heights = jax.random.uniform(jax.random.fold_in(jax.random.fold_in(rng, 6), dim), (parts,), jnp.float32, smallest / len(pieces), top_value / len(pieces))
        return jnp.repeat(jnp.exp(heights), extent[dim] // parts).reshape((-1,) + (1,) * (len(extent) - dim - 1))

    level = one(*pieces[0])
    for cut in pieces[1:]:
        level = level * one(*cut)
    return level


def split_up(number_of, total, most, skew):
    portions = [(1 << 20) // math.isqrt(grade ** skew) + 1 for grade in range(2, number_of + 1)]
    surplus, counts = total - most - (number_of - 1), [1] * (number_of - 1)
    while surplus > 0:
        movable = [i for i in range(number_of - 1) if counts[i] < most]
        pool, left = sum([portions[i] for i in movable]), surplus
        for i in movable:
            more = min(most - counts[i], max(1, left * portions[i] // pool), surplus)
            counts[i] = counts[i] + more
            surplus = surplus - more
    return np.array([most] + counts)


def uneven_parts(stream_key, number_of, total, bound, skew):
    if number_of == 2:
        one = jax.random.randint(stream_key, (), max(1, total - bound), min(bound, total - 1) + 1)
        return jnp.stack([one, total - one])
    sizes = jnp.asarray(split_up(number_of, total, bound, skew), jnp.int32)
    twos = (number_of - 1) // 2
    source_of, sink = sizes[1:1 + 2 * twos:2], sizes[2:2 + 2 * twos:2]
    margin = jnp.minimum(source_of - 1, bound - sink)
    moved = jax.random.randint(jax.random.fold_in(stream_key, 1), (twos,), 0, 1 << 20) % (margin + 1)
    sizes = sizes.at[1:1 + 2 * twos:2].set(source_of - moved).at[2:2 + 2 * twos:2].set(sink + moved)
    return sizes[jax.random.permutation(jax.random.fold_in(stream_key, 2), number_of)]


def centred(stream_key, extent, deviation, bound, pieces=(), kind=jnp.bfloat16):
    values = deviation * jax.random.normal(stream_key, extent, jnp.float32)
    if pieces:
        values = values * steps_of(stream_key, extent, pieces, -0.22, 0.18)
    return jnp.clip(values, -bound, bound).astype(kind)


def setup_inputs(seed: int = 0) -> dict:
    keys = jax.random.split(jax.random.key(seed), 10)
    return {
        "image_in": centred(keys[0], (IMAGES, ROWS_ALL, COLS, C), 1.0, 6.0, ((0, 8), (1, 4))),
        "cotangent": centred(keys[1], (IMAGES, ROWS_ALL, COLS, C), 1.0, 6.0, ((0, 8), (1, 4))),
        "conv1_w": centred(keys[2], (3, 3, C, C), (9 * C) ** -0.5, 0.1875),
        "conv2_w": centred(keys[3], (3, 3, C, C), (9 * C) ** -0.5, 0.1875),
        "norm1_gain": jnp.clip(1.0 + 0.1 * jax.random.normal(keys[4], (C,), jnp.float32), 0.5, 1.5),
        "norm1_shift": centred(keys[5], (C,), 0.5, 3.0, (), jnp.float32),
        "norm2_gain": jnp.clip(1.0 + 0.1 * jax.random.normal(keys[6], (C,), jnp.float32), 0.5, 1.5),
        "norm2_shift": centred(keys[7], (C,), 0.5, 3.0, (), jnp.float32),
        "strip_rows": jax.vmap(lambda own: uneven_parts(own, N_STRIP, HEIGHT, CAP, 2))(jax.random.split(keys[8], IMAGES)).reshape((IMAGES, N_STRIP)).astype(jnp.int32),
    }


EPSILON = 1e-06

def silu_slope(pre_act):
    logistic = jax.nn.sigmoid(pre_act)
    return logistic * (1.0 + pre_act * (1.0 - logistic))

def group_average(values):
    per_channel = lax.optimization_barrier(jnp.sum(values, axis=(0, 1)))
    grouped = per_channel.reshape(GROUPS, -1)
    return jnp.repeat(lax.optimization_barrier(jnp.sum(grouped, axis=1)) / (values.shape[0] * values.shape[1] * grouped.shape[1]), grouped.shape[1])

def group_norm(values, gain, shift):
    mean_val = group_average(values)
    centered = values - mean_val
    variance = group_average(centered * centered)
    inv_std = lax.rsqrt(variance + EPSILON)
    normed = centered * inv_std
    return (normed, normed * gain + shift, inv_std)

def norm_backward(grad_pre, normed, gain, inv_std):
    scaled = grad_pre * gain
    return inv_std * (scaled - group_average(scaled) - normed * group_average(scaled * normed))

def convolve(padded, kernel, row_count, col_count):
    running = jnp.zeros((row_count * col_count, kernel.shape[3]), jnp.float32)
    for tap_row in range(3):
        for tap_col in range(3):
            window = padded[tap_row:tap_row + row_count, tap_col:tap_col + col_count].reshape(row_count * col_count, -1)
            running = running + jnp.dot(window, kernel[tap_row, tap_col], preferred_element_type=jnp.float32)
    return running.reshape(row_count, col_count, -1)

def kernel_grad(padded, upstream, row_count, col_count):
    flat_up = upstream.reshape(row_count * col_count, -1)
    tap_grads = []
    for tap_row in range(3):
        for tap_col in range(3):
            window = padded[tap_row:tap_row + row_count, tap_col:tap_col + col_count].reshape(row_count * col_count, -1)
            tap_grads.append(lax.dot_general(window, flat_up, (((0,), (0,)), ((), ())), preferred_element_type=jnp.float32))
    return jnp.stack(tap_grads).reshape(-1, flat_up.shape[1])

def spread_back(upstream, kernel, row_count, col_count):
    flat_up = upstream.reshape(row_count * col_count, -1)
    gradient = jnp.zeros((row_count + 2, col_count + 2, kernel.shape[2]), jnp.float32)
    for tap_row in range(3):
        for tap_col in range(3):
            product = lax.dot_general(flat_up, kernel[tap_row, tap_col], (((1,), (1,)), ((), ())), preferred_element_type=jnp.float32)
            product = product.reshape(row_count, col_count, -1)
            gradient = gradient + jnp.pad(product, ((tap_row, 2 - tap_row), (tap_col, 2 - tap_col), (0, 0)))
    return gradient

def compact_index(lengths):
    lengths = lengths.astype(jnp.int32)
    ends = jnp.cumsum(lengths).astype(jnp.int32)
    starts = ends - lengths
    position = jnp.arange(HEIGHT, dtype=jnp.int32)
    owner = lax.optimization_barrier(jnp.sum((position[:, None] >= ends[None, :]).astype(jnp.int32), axis=1)).astype(jnp.int32)
    strip_ids = jnp.arange(N_STRIP, dtype=jnp.int32)
    offset = position - lax.optimization_barrier(jnp.sum(jnp.where(owner[:, None] == strip_ids[None, :], starts[None, :], 0), axis=1)).astype(jnp.int32)
    return (owner * CAP + offset).astype(jnp.int32)

def reference(image_in, cotangent, conv1_w, conv2_w, norm1_gain, norm1_shift, norm2_gain, norm2_shift, strip_rows):

    def one_image(operands):
        source, upstream, lengths = operands
        row_ids = compact_index(lengths)
        inputs = source[row_ids].astype(jnp.float32)
        grad_out = upstream[row_ids]
        normed_one, pre_one, inv_one = group_norm(inputs, norm1_gain, norm1_shift)
        act_one = jax.nn.silu(pre_one).astype(jnp.bfloat16)
        padded_one = jnp.pad(act_one, ((1, 1), (1, 1), (0, 0)))
        hidden = convolve(padded_one, conv1_w, HEIGHT, COLS)
        normed_two, pre_two, inv_two = group_norm(hidden, norm2_gain, norm2_shift)
        act_two = jax.nn.silu(pre_two).astype(jnp.bfloat16)
        padded_two = jnp.pad(act_two, ((1, 1), (1, 1), (0, 0)))
        grad_two = kernel_grad(padded_two, grad_out, HEIGHT, COLS)
        back_two = spread_back(grad_out, conv2_w, HEIGHT, COLS)[1:-1, 1:-1]
        dpre_two = back_two * silu_slope(pre_two)
        hidden_grad = norm_backward(dpre_two, normed_two, norm2_gain, inv_two).astype(jnp.bfloat16)
        grad_one = kernel_grad(padded_one, hidden_grad, HEIGHT, COLS)
        back_one = spread_back(hidden_grad, conv1_w, HEIGHT, COLS)[1:-1, 1:-1]
        dpre_one = back_one * silu_slope(pre_one)
        branch = norm_backward(dpre_one, normed_one, norm1_gain, inv_one)
        result = (grad_out.astype(jnp.float32) + branch).astype(jnp.bfloat16)
        full = jnp.zeros((ROWS_ALL, COLS, C), jnp.bfloat16).at[row_ids].set(result)
        norm_terms = jnp.stack([lax.optimization_barrier(jnp.sum(dpre_one * normed_one, axis=(0, 1))), lax.optimization_barrier(jnp.sum(dpre_one, axis=(0, 1))), lax.optimization_barrier(jnp.sum(dpre_two * normed_two, axis=(0, 1))), lax.optimization_barrier(jnp.sum(dpre_two, axis=(0, 1)))])
        return (full, grad_one, grad_two, norm_terms)
    image_grad, grads_one, grads_two, norm_terms = lax.map(one_image, (image_in, cotangent, strip_rows))
    return (image_grad, lax.optimization_barrier(jnp.sum(grads_one, axis=0)), lax.optimization_barrier(jnp.sum(grads_two, axis=0)), lax.optimization_barrier(jnp.sum(norm_terms, axis=0)))
```

```python
import functools

import jax
import jax.numpy as jnp
from jax import lax
from jax.experimental import pallas as pl
from jax.experimental.pallas import tpu as pltpu
from jax.sharding import PartitionSpec as P

GROUPS = 32
EPSILON = 1e-06
F32 = jnp.float32
BF16 = jnp.bfloat16
MESH = pl.DeviceIdType.MESH


def ceil_to(value, unit):
    return -(-value // unit) * unit


def sigmoid(z):
    return 0.5 * jnp.tanh(0.5 * z) + 0.5


def group_sum(block, size):
    lanes = block.shape[1]
    lane = lax.broadcasted_iota(jnp.int32, block.shape, 1)
    step = 1
    while step < size:
        upper = pltpu.roll(block, lanes - step, 1)
        lower = pltpu.roll(block, step, 1)
        block = block + jnp.where((lane & step) == 0, upper, lower)
        step *= 2
    return block


def fold(values):
    return jnp.sum(values.reshape(values.shape[0] // 8, 8, values.shape[1]), axis=0)


def flat(block):
    return jnp.broadcast_to(jnp.sum(block, axis=0, keepdims=True), block.shape)


def by_row(parts):
    row = lax.broadcasted_iota(jnp.int32, parts[0].shape, 0)
    out = jnp.zeros_like(parts[0])
    for k, part in enumerate(parts):
        out = jnp.where(row == k, part, out)
    return out


def kernel(
    n,
    m,
    rows_out,
    quota,
    len_ref,
    x_ref,
    g_ref,
    w1_ref,
    w2_ref,
    gain1_ref,
    shift1_ref,
    gain2_ref,
    shift2_ref,
    out_ref,
    grad1_ref,
    grad2_ref,
    norm_ref,
    buf1,
    buf2,
    bufd,
    hidden,
    back,
    act2,
    dh,
    gt,
    wp,
    acc,
    full,
    edge,
    halo,
    xbuf,
    nbuf,
    rs,
    got1,
    part,
    got2,
    ag,
    halo_send,
    halo_recv,
    x_send,
    x_recv,
    n_send,
    n_recv,
    s1_send,
    s1_recv,
    s2_send,
    s2_recv,
    s3_send,
    s3_recv,
):
    _, slots, cols, chans = x_ref.shape
    size = chans // GROUPS
    me = lax.axis_index("strip")
    img = lax.axis_index("img")
    length = len_ref[0, 0]
    last = jnp.maximum(length - 1, 0)
    height = slots * n // 2
    cells = float(height * cols * size)

    barrier = pltpu.get_barrier_semaphore()
    for d in range(1, n):
        pl.semaphore_signal(
            barrier, inc=1, device_id={"strip": lax.rem(me + d, n)}, device_id_type=MESH
        )
    for d in range(1, m):
        pl.semaphore_signal(
            barrier, inc=1, device_id={"img": lax.rem(img + d, m)}, device_id_type=MESH
        )

    def send_halo(kind, first, last):
        below = pltpu.make_async_remote_copy(
            src_ref=last,
            dst_ref=halo.at[kind, 0],
            send_sem=halo_send.at[kind, 0],
            recv_sem=halo_recv.at[kind, 0],
            device_id={"strip": lax.rem(me + 1, n)},
            device_id_type=MESH,
        )
        above = pltpu.make_async_remote_copy(
            src_ref=first,
            dst_ref=halo.at[kind, 1],
            send_sem=halo_send.at[kind, 1],
            recv_sem=halo_recv.at[kind, 1],
            device_id={"strip": lax.rem(me + n - 1, n)},
            device_id_type=MESH,
        )
        below.start()
        above.start()
        return [below, above]

    def send_block(kind, block):
        xbuf[kind, me] = block
        copies = []
        for d in range(1, n):
            copy = pltpu.make_async_remote_copy(
                src_ref=xbuf.at[kind, me],
                dst_ref=xbuf.at[kind, me],
                send_sem=x_send.at[kind, d - 1],
                recv_sem=x_recv.at[kind, d - 1],
                device_id={"strip": lax.rem(me + d, n)},
                device_id_type=MESH,
            )
            copy.start()
            copies.append(copy)
        return copies

    def wait_all(copies):
        for copy in copies:
            copy.wait()

    def live(row):
        return jnp.full((cols, chans), row, jnp.int32) < length

    zero8 = jnp.zeros((8, chans), F32)

    def local_stats(load):
        def add(r, total):
            return total + fold(jnp.where(live(r), load(r), 0.0))

        total = lax.fori_loop(0, slots, add, zero8, unroll=2)
        count = (jnp.full((8, chans), length, jnp.int32) * (cols * size)).astype(F32)
        mean = group_sum(flat(total), size) / count
        one = mean[0:1]

        def spread(r, total):
            centered = jnp.where(live(r), load(r) - one, 0.0)
            return total + fold(centered * centered)

        spread_sum = lax.fori_loop(0, slots, spread, zero8, unroll=2)
        return by_row([count, mean, group_sum(flat(spread_sum), size)])

    def joined_stats(kind):
        count = xbuf[kind, 0, 0:1]
        weighted = count * xbuf[kind, 0, 1:2]
        total = count
        for k in range(1, n):
            count = xbuf[kind, k, 0:1]
            total = total + count
            weighted = weighted + count * xbuf[kind, k, 1:2]
        mean = weighted / total
        spread = jnp.zeros_like(mean)
        for k in range(n):
            delta = xbuf[kind, k, 1:2] - mean
            spread = spread + (xbuf[kind, k, 2:3] + xbuf[kind, k, 0:1] * delta * delta)
        return mean, lax.rsqrt(spread / cells + EPSILON)

    def joined_sums(kind):
        total = xbuf[kind, 0]
        for k in range(1, n):
            total = total + xbuf[kind, k]
        return total

    def means_of(sums, gain):
        both = group_sum(sums * gain, size) / cells
        return both[0:1], both[1:2]

    column = lax.broadcasted_iota(jnp.int32, (cols, chans), 0)
    has_above = jnp.where(me > 0, 1, 0)
    has_below = jnp.where(me < n - 1, 1, 0)

    def build(buf, kind, load, change):
        def one_row(i, carry):
            r = i - 1
            own = load(jnp.clip(r, 0, slots - 1)).astype(F32)
            at = jnp.full((cols, chans), r, jnp.int32)
            value = jnp.where(at < 0, halo[kind, 0].astype(F32), own)
            value = jnp.where(at == length, halo[kind, 1].astype(F32), value)
            keep = jnp.where(at < 0, has_above, jnp.where(at == length, has_below, 1))
            keep = jnp.where(at > length, 0, keep)
            value = jnp.where(keep > 0, change(value), 0.0)
            before = jnp.where(column == 0, 0.0, pltpu.roll(value, 1, 0))
            after = jnp.where(column == cols - 1, 0.0, pltpu.roll(value, cols - 1, 0))
            buf[i, :, 0:chans] = before.astype(BF16)
            buf[i, :, chans : 2 * chans] = value.astype(BF16)
            buf[i, :, 2 * chans : 3 * chans] = after.astype(BF16)
            return carry

        lax.fori_loop(0, slots + 2, one_row, 0, unroll=2)
        buf[slots + 2] = jnp.zeros((cols, 3 * chans), BF16)
        buf[slots + 3] = jnp.zeros((cols, 3 * chans), BF16)

    def load_forward(w_ref):
        for j in range(4):
            for b in range(3):
                at = (j * 3 + b) * chans
                for t in range(2):
                    a = j - t
                    tap = w_ref[a, b] if 0 <= a <= 2 else jnp.zeros((chans, chans), BF16)
                    wp[at : at + chans, t * chans : (t + 1) * chans] = tap

    def load_backward(w_ref):
        for j in range(4):
            for b in range(3):
                at = (j * 3 + b) * chans
                for t in range(2):
                    a = j - t
                    if 0 <= a <= 2:
                        tap = w_ref[2 - a, 2 - b].astype(F32).T.astype(BF16)
                    else:
                        tap = jnp.zeros((chans, chans), BF16)
                    wp[at : at + chans, t * chans : (t + 1) * chans] = tap

    pairs = 4

    def convolve(buf, out):
        def step(q, carry):
            base = q * (2 * pairs)
            pieces = []
            for p in range(pairs):
                pieces.append(
                    jnp.concatenate([buf[base + (2 * p + j)] for j in range(4)], axis=1)
                )
            result = jnp.dot(
                jnp.concatenate(pieces, axis=0), wp[...], preferred_element_type=F32
            )
            for p in range(pairs):
                for t in range(2):
                    out[base + (2 * p + t)] = result[
                        p * cols : (p + 1) * cols, t * chans : (t + 1) * chans
                    ]
            return carry

        lax.fori_loop(0, slots // (2 * pairs), step, 0)

    def kernel_grad(buf):
        acc[...] = jnp.zeros_like(acc)
        rows = 4

        def step(q, carry):
            left = jnp.concatenate(
                [
                    jnp.concatenate([gt[q * rows + (k + 2 - a)] for k in range(rows)], axis=1)
                    for a in range(3)
                ],
                axis=0,
            )
            right = jnp.concatenate([buf[q * rows + k] for k in range(rows)], axis=0)
            acc[...] += jnp.dot(left, right, preferred_element_type=F32)
            return carry

        lax.fori_loop(0, (slots + 4) // rows, step, 0)
        for a in range(3):
            for b in range(3):
                at = (a * 3 + b) * chans
                full[at : at + chans] = acc[
                    a * chans : (a + 1) * chans, b * chans : (b + 1) * chans
                ].T

    def scatter_strips(k):
        for i in range(m):
            for s in range(n):
                low = min(s * quota, rows_out)
                high = min(low + quota, rows_out)
                if high > low:
                    rs[k, i, s, 0 : high - low] = full[i * rows_out + low : i * rows_out + high]
                if high - low < quota:
                    rs[k, i, s, high - low : quota] = jnp.zeros(
                        (quota - (high - low), chans), F32
                    )
        copies = []
        for d in range(1, n):
            peer = lax.rem(me + d, n)
            copy = pltpu.make_async_remote_copy(
                src_ref=rs.at[k, :, peer],
                dst_ref=got1.at[k, d - 1],
                send_sem=s1_send.at[k, d - 1],
                recv_sem=s1_recv.at[k, d - 1],
                device_id={"strip": peer},
                device_id_type=MESH,
            )
            copy.start()
            copies.append(copy)
        return copies

    def scatter_images(k, before):
        wait_all(before)

        def add(i, carry):
            total = rs[k, i, me]
            for d in range(n - 1):
                total = total + got1[k, d, i]
            part[k, i] = total
            return carry

        lax.fori_loop(0, m, add, 0)
        copies = []
        for d in range(1, m):
            peer = lax.rem(img + d, m)
            copy = pltpu.make_async_remote_copy(
                src_ref=part.at[k, peer],
                dst_ref=got2.at[k, d - 1],
                send_sem=s2_send.at[k, d - 1],
                recv_sem=s2_recv.at[k, d - 1],
                device_id={"img": peer},
                device_id_type=MESH,
            )
            copy.start()
            copies.append(copy)
        return copies

    def gather_strips(k, before):
        wait_all(before)
        total = part[k, img]
        for d in range(m - 1):
            total = total + got2[k, d]
        ag[k, me] = total
        copies = []
        for d in range(1, n):
            copy = pltpu.make_async_remote_copy(
                src_ref=ag.at[k, me],
                dst_ref=ag.at[k, me],
                send_sem=s3_send.at[k, d - 1],
                recv_sem=s3_recv.at[k, d - 1],
                device_id={"strip": lax.rem(me + d, n)},
                device_id_type=MESH,
            )
            copy.start()
            copies.append(copy)
        return copies

    def finish_grad(k, before, target):
        wait_all(before)
        for s in range(n):
            low = min(s * quota, rows_out)
            high = min(low + quota, rows_out)
            if high > low:
                target[low:high] = ag[k, s, 0 : high - low]

    edge[0] = x_ref[0, last]
    edge[1] = g_ref[0, last]
    block = local_stats(lambda r: x_ref[0, r].astype(F32))
    pl.semaphore_wait(barrier, n - 1 + m - 1)
    stats1 = send_block(0, block)
    halo_x = send_halo(0, x_ref.at[0, 0], edge.at[0])
    halo_g = send_halo(1, g_ref.at[0, 0], edge.at[1])

    load_forward(w1_ref)
    for k in (0, 1, slots + 2, slots + 3, slots + 4, slots + 5):
        gt[k] = jnp.zeros((chans, cols), BF16)

    def turn_cotangent(r, carry):
        gt[r + 2] = jnp.where(live(r), g_ref[0, r].astype(F32), 0.0).T.astype(BF16)
        return carry

    lax.fori_loop(0, slots, turn_cotangent, 0, unroll=2)
    wait_all(halo_g)
    build(bufd, 1, lambda r: g_ref[0, r], lambda v: v)
    wait_all(halo_x)
    wait_all(stats1)

    gain1, shift1 = gain1_ref[...], shift1_ref[...]
    gain2, shift2 = gain2_ref[...], shift2_ref[...]
    mean1, inv1 = joined_stats(0)

    def act_one(v):
        pre = (v - mean1) * inv1 * gain1 + shift1
        return pre * sigmoid(pre)

    build(buf1, 0, lambda r: x_ref[0, r], act_one)
    convolve(buf1, hidden)
    stats2 = send_block(1, local_stats(lambda r: hidden[r]))
    load_backward(w2_ref)
    convolve(bufd, back)
    wait_all(stats2)
    mean2, inv2 = joined_stats(1)

    def slope_two(r, carry):
        sum_plain, sum_cross = carry
        normed = (hidden[r] - mean2) * inv2
        pre = normed * gain2 + shift2
        logistic = sigmoid(pre)
        act2[r] = (pre * logistic).astype(BF16)
        slope = logistic * (1.0 + pre * (1.0 - logistic))
        dpre = jnp.where(live(r), back[r] * slope, 0.0)
        back[r] = dpre
        return sum_plain + fold(dpre), sum_cross + fold(dpre * normed)

    sum_plain, sum_cross = lax.fori_loop(0, slots, slope_two, (zero8, zero8))
    edge[2] = act2[last]
    halo_a = send_halo(2, act2.at[0], edge.at[2])
    sums2 = send_block(2, by_row([flat(sum_plain), flat(sum_cross)]))
    load_backward(w1_ref)
    wait_all(halo_a)
    build(buf2, 2, lambda r: act2[r], lambda v: v)
    kernel_grad(buf2)
    stage = scatter_strips(1)
    wait_all(sums2)
    total2 = joined_sums(2)
    mean_plain2, mean_cross2 = means_of(total2, gain2)

    def hidden_grad(r, carry):
        normed = (hidden[r] - mean2) * inv2
        value = inv2 * (back[r] * gain2 - mean_plain2 - normed * mean_cross2)
        value = jnp.where(live(r), value, 0.0)
        dh[r] = value.astype(BF16)
        gt[r + 2] = value.T.astype(BF16)
        return carry

    lax.fori_loop(0, slots, hidden_grad, 0)
    edge[3] = dh[last]
    halo_d = send_halo(3, dh.at[0], edge.at[3])
    kernel_grad(buf1)
    stage_one = scatter_strips(0)
    stage = scatter_images(1, stage)
    wait_all(halo_d)
    build(bufd, 3, lambda r: dh[r], lambda v: v)
    convolve(bufd, back)
    stage = gather_strips(1, stage)

    def slope_one(r, carry):
        sum_plain, sum_cross = carry
        normed = (x_ref[0, r].astype(F32) - mean1) * inv1
        pre = normed * gain1 + shift1
        logistic = sigmoid(pre)
        slope = logistic * (1.0 + pre * (1.0 - logistic))
        dpre = jnp.where(live(r), back[r] * slope, 0.0)
        back[r] = dpre
        return sum_plain + fold(dpre), sum_cross + fold(dpre * normed)

    sum_plain, sum_cross = lax.fori_loop(0, slots, slope_one, (zero8, zero8))
    sums1 = send_block(3, by_row([flat(sum_plain), flat(sum_cross)]))
    stage_one = scatter_images(0, stage_one)
    wait_all(sums1)
    total1 = joined_sums(3)
    mean_plain1, mean_cross1 = means_of(total1, gain1)

    def spread8(row):
        return jnp.broadcast_to(row, (8, chans))

    nbuf[img] = by_row(
        [spread8(total1[1:2]), spread8(total1[0:1]), spread8(total2[1:2]), spread8(total2[0:1])]
    )
    norms = []
    for d in range(1, m):
        copy = pltpu.make_async_remote_copy(
            src_ref=nbuf.at[img],
            dst_ref=nbuf.at[img],
            send_sem=n_send.at[d - 1],
            recv_sem=n_recv.at[d - 1],
            device_id={"img": lax.rem(img + d, m)},
            device_id_type=MESH,
        )
        copy.start()
        norms.append(copy)

    def image_grad(r, carry):
        normed = (x_ref[0, r].astype(F32) - mean1) * inv1
        branch = inv1 * (back[r] * gain1 - mean_plain1 - normed * mean_cross1)
        value = g_ref[0, r].astype(F32) + branch
        out_ref[0, r] = jnp.where(live(r), value, 0.0).astype(BF16)
        return carry

    lax.fori_loop(0, slots, image_grad, 0, unroll=2)
    stage_one = gather_strips(0, stage_one)
    finish_grad(1, stage, grad2_ref)
    wait_all(norms)
    total = nbuf[0]
    for i in range(1, m):
        total = total + nbuf[i]
    norm_ref[...] = total[0:4]
    finish_grad(0, stage_one, grad1_ref)


def body(
    image_in,
    cotangent,
    conv1_w,
    conv2_w,
    norm1_gain,
    norm1_shift,
    norm2_gain,
    norm2_shift,
    strip_rows,
):
    n = lax.axis_size("strip")
    m = lax.axis_size("img")
    _, slots, cols, chans = image_in.shape
    rows_out = 9 * chans // m
    quota = ceil_to(-(-rows_out // n), 8)
    vmem = pl.BlockSpec(memory_space=pltpu.VMEM)
    padded = slots + 4
    scratch = [
        pltpu.VMEM((padded, cols, 3 * chans), BF16),
        pltpu.VMEM((padded, cols, 3 * chans), BF16),
        pltpu.VMEM((padded, cols, 3 * chans), BF16),
        pltpu.VMEM((slots, cols, chans), F32),
        pltpu.VMEM((slots, cols, chans), F32),
        pltpu.VMEM((slots, cols, chans), BF16),
        pltpu.VMEM((slots, cols, chans), BF16),
        pltpu.VMEM((slots + 6, chans, cols), BF16),
        pltpu.VMEM((12 * chans, 2 * chans), BF16),
        pltpu.VMEM((3 * chans, 3 * chans), F32),
        pltpu.VMEM((9 * chans, chans), F32),
        pltpu.VMEM((4, cols, chans), BF16),
        pltpu.VMEM((4, 2, cols, chans), BF16),
        pltpu.VMEM((4, n, 8, chans), F32),
        pltpu.VMEM((m, 8, chans), F32),
        pltpu.VMEM((2, m, n, quota, chans), F32),
        pltpu.VMEM((2, n - 1, m, quota, chans), F32),
        pltpu.VMEM((2, m, quota, chans), F32),
        pltpu.VMEM((2, m - 1, quota, chans), F32),
        pltpu.VMEM((2, n, quota, chans), F32),
        pltpu.SemaphoreType.DMA((4, 2)),
        pltpu.SemaphoreType.DMA((4, 2)),
        pltpu.SemaphoreType.DMA((4, n - 1)),
        pltpu.SemaphoreType.DMA((4, n - 1)),
        pltpu.SemaphoreType.DMA((m - 1,)),
        pltpu.SemaphoreType.DMA((m - 1,)),
        pltpu.SemaphoreType.DMA((2, n - 1)),
        pltpu.SemaphoreType.DMA((2, n - 1)),
        pltpu.SemaphoreType.DMA((2, m - 1)),
        pltpu.SemaphoreType.DMA((2, m - 1)),
        pltpu.SemaphoreType.DMA((2, n - 1)),
        pltpu.SemaphoreType.DMA((2, n - 1)),
    ]
    return pl.pallas_call(
        functools.partial(kernel, n, m, rows_out, quota),
        out_shape=(
            jax.ShapeDtypeStruct(image_in.shape, BF16),
            jax.ShapeDtypeStruct((rows_out, chans), F32),
            jax.ShapeDtypeStruct((rows_out, chans), F32),
            jax.ShapeDtypeStruct((4, chans), F32),
        ),
        in_specs=[pl.BlockSpec(memory_space=pltpu.SMEM)] + [vmem] * 8,
        out_specs=(vmem,) * 4,
        scratch_shapes=scratch,
        compiler_params=pltpu.CompilerParams(
            collective_id=0, has_side_effects=True, vmem_limit_bytes=56 * 1024 * 1024
        ),
    )(
        strip_rows,
        image_in,
        cotangent,
        conv1_w,
        conv2_w,
        norm1_gain.reshape(1, chans),
        norm1_shift.reshape(1, chans),
        norm2_gain.reshape(1, chans),
        norm2_shift.reshape(1, chans),
    )


def solution(mesh):
    placed = (
        P("img", "strip", None, None),
        P("img", "strip", None, None),
        P(),
        P(),
        P(),
        P(),
        P(),
        P(),
        P("img", "strip"),
    )
    return jax.shard_map(
        body,
        mesh=mesh,
        in_specs=placed,
        out_specs=(P("img", "strip", None, None), P("img", None), P("img", None), P()),
        check_vma=False,
    )
```

```python
import functools

import jax
import jax.numpy as jnp
from jax import lax
from jax.experimental import pallas as pl
from jax.experimental.pallas import tpu as pltpu
from jax.sharding import PartitionSpec as P

GROUPS = 32
EPSILON = 1e-06
F32 = jnp.float32
BF16 = jnp.bfloat16
MESH = pl.DeviceIdType.MESH


def sigmoid(z):
    return 0.5 * jnp.tanh(0.5 * z) + 0.5


def group_sum(block, size):
    lanes = block.shape[1]
    lane = lax.broadcasted_iota(jnp.int32, block.shape, 1)
    step = 1
    while step < size:
        upper = pltpu.roll(block, lanes - step, 1)
        lower = pltpu.roll(block, step, 1)
        block = block + jnp.where((lane & step) == 0, upper, lower)
        step *= 2
    return block


def fold(values):
    return jnp.sum(values.reshape(values.shape[0] // 8, 8, values.shape[1]), axis=0)


def flat(block):
    return jnp.broadcast_to(jnp.sum(block, axis=0, keepdims=True), block.shape)


def by_row(parts):
    row = lax.broadcasted_iota(jnp.int32, parts[0].shape, 0)
    out = jnp.zeros_like(parts[0])
    for k, part in enumerate(parts):
        out = jnp.where(row == k, part, out)
    return out


def kernel(
    n,
    m,
    rows_out,
    len_ref,
    x_ref,
    g_ref,
    w1_ref,
    w2_ref,
    gain1_ref,
    shift1_ref,
    gain2_ref,
    shift2_ref,
    out_ref,
    grad1_ref,
    grad2_ref,
    norm_ref,
    buf1,
    buf2,
    bufd,
    hidden,
    back,
    act2,
    dh,
    gt,
    wp,
    acc,
    full,
    edge,
    halo,
    xbuf,
    nbuf,
    rs,
    got,
    ag,
    corr,
    halo_send,
    halo_recv,
    x_send,
    x_recv,
    n_send,
    n_recv,
    s1_send,
    s1_recv,
    s2_send,
    s2_recv,
):
    _, slots, cols, chans = x_ref.shape
    size = chans // GROUPS
    me = lax.axis_index("strip")
    img = lax.axis_index("img")
    length = len_ref[0, 0]
    last = jnp.maximum(length - 1, 0)
    height = slots * n // 2
    cells = float(height * cols * size)

    barrier = pltpu.get_barrier_semaphore()
    for d in range(1, n):
        pl.semaphore_signal(
            barrier, inc=1, device_id={"strip": lax.rem(me + d, n)}, device_id_type=MESH
        )
    for d in range(1, m):
        pl.semaphore_signal(
            barrier, inc=1, device_id={"img": lax.rem(img + d, m)}, device_id_type=MESH
        )

    def send_halo(kind, first, last):
        below = pltpu.make_async_remote_copy(
            src_ref=last,
            dst_ref=halo.at[kind, 0],
            send_sem=halo_send.at[kind, 0],
            recv_sem=halo_recv.at[kind, 0],
            device_id={"strip": lax.rem(me + 1, n)},
            device_id_type=MESH,
        )
        above = pltpu.make_async_remote_copy(
            src_ref=first,
            dst_ref=halo.at[kind, 1],
            send_sem=halo_send.at[kind, 1],
            recv_sem=halo_recv.at[kind, 1],
            device_id={"strip": lax.rem(me + n - 1, n)},
            device_id_type=MESH,
        )
        pl.when(me < n - 1)(below.start)
        pl.when(me > 0)(above.start)

        def wait():
            @pl.when(me < n - 1)
            def _():
                below.wait_send()
                above.wait_recv()

            @pl.when(me > 0)
            def _():
                above.wait_send()
                below.wait_recv()

        return wait

    def send_block(kind, block):
        xbuf[kind, me] = block
        copies = []
        for d in range(1, n):
            copy = pltpu.make_async_remote_copy(
                src_ref=xbuf.at[kind, me],
                dst_ref=xbuf.at[kind, me],
                send_sem=x_send.at[kind, d - 1],
                recv_sem=x_recv.at[kind, d - 1],
                device_id={"strip": lax.rem(me + d, n)},
                device_id_type=MESH,
            )
            copy.start()
            copies.append(copy)
        return copies

    def wait_all(copies):
        for copy in copies:
            copy.wait()

    def live(row):
        return jnp.full((cols, chans), row, jnp.int32) < length

    zero8 = jnp.zeros((8, chans), F32)

    def local_stats(load):
        def add(r, total):
            return total + fold(jnp.where(live(r), load(r), 0.0))

        total = lax.fori_loop(0, slots, add, zero8, unroll=2)
        count = (jnp.full((8, chans), length, jnp.int32) * (cols * size)).astype(F32)
        mean = group_sum(flat(total), size) / count
        one = mean[0:1]

        def spread(r, total):
            centered = jnp.where(live(r), load(r) - one, 0.0)
            return total + fold(centered * centered)

        spread_sum = lax.fori_loop(0, slots, spread, zero8, unroll=2)
        return by_row([count, mean, group_sum(flat(spread_sum), size)])

    def joined_stats(kind):
        count = xbuf[kind, 0, 0:1]
        weighted = count * xbuf[kind, 0, 1:2]
        total = count
        for k in range(1, n):
            count = xbuf[kind, k, 0:1]
            total = total + count
            weighted = weighted + count * xbuf[kind, k, 1:2]
        mean = weighted / total
        spread = jnp.zeros_like(mean)
        for k in range(n):
            delta = xbuf[kind, k, 1:2] - mean
            spread = spread + (xbuf[kind, k, 2:3] + xbuf[kind, k, 0:1] * delta * delta)
        return mean, lax.rsqrt(spread / cells + EPSILON)

    def joined_sums(kind):
        total = xbuf[kind, 0]
        for k in range(1, n):
            total = total + xbuf[kind, k]
        return total

    def means_of(sums, gain):
        both = group_sum(sums * gain, size) / cells
        return both[0:1], both[1:2]

    column = lax.broadcasted_iota(jnp.int32, (cols, chans), 0)
    has_above = jnp.where(me > 0, 1, 0)
    has_below = jnp.where(me < n - 1, 1, 0)

    def shifted(value):
        before = jnp.where(column == 0, 0.0, pltpu.roll(value, 1, 0))
        after = jnp.where(column == cols - 1, 0.0, pltpu.roll(value, cols - 1, 0))
        return before.astype(BF16), value.astype(BF16), after.astype(BF16)

    def put(buf, i, value):
        for b, piece in enumerate(shifted(value)):
            buf[i, :, b * chans : (b + 1) * chans] = piece

    def clear(buf, i):
        buf[i] = jnp.zeros((cols, 3 * chans), BF16)

    def build(buf, load):
        def one_row(r, carry):
            put(buf, r + 1, load(r))
            return carry

        lax.fori_loop(0, slots, one_row, 0, unroll=2)
        clear(buf, 0)
        clear(buf, slots + 1)

    def build_joined(buf, kind, load, change):
        def one_row(i, carry):
            r = i - 1
            own = load(jnp.clip(r, 0, slots - 1)).astype(F32)
            at = jnp.full((cols, chans), r, jnp.int32)
            value = jnp.where(at < 0, halo[kind, 0].astype(F32), own)
            value = jnp.where(at == length, halo[kind, 1].astype(F32), value)
            keep = jnp.where(at < 0, has_above, jnp.where(at == length, has_below, 1))
            keep = jnp.where(at > length, 0, keep)
            put(buf, i, jnp.where(keep > 0, change(value), 0.0))
            return carry

        lax.fori_loop(0, slots + 2, one_row, 0, unroll=2)

    def arrived(kind):
        flags = (has_above, has_below)
        return [
            jnp.concatenate(
                shifted(
                    jnp.where(
                        jnp.full((cols, chans), flags[e], jnp.int32) > 0,
                        halo[kind, e].astype(F32),
                        0.0,
                    )
                ),
                axis=1,
            )
            for e in range(2)
        ]

    def edge_terms(kind, w):
        top, bottom = arrived(kind)
        taps = 3 * chans
        corr[0] = jnp.dot(top, wp[w, 0:taps, 0:chans], preferred_element_type=F32)
        corr[1] = jnp.dot(bottom, wp[w, 2 * taps : 3 * taps, 0:chans], preferred_element_type=F32)

    def with_edges(r):
        at = jnp.full((cols, chans), r, jnp.int32)
        value = back[r] + jnp.where(at == 0, corr[0], 0.0)
        return value + jnp.where(at == last, corr[1], 0.0)

    def load_forward(w, w_ref):
        for j in range(4):
            for b in range(3):
                at = (j * 3 + b) * chans
                for t in range(2):
                    a = j - t
                    tap = w_ref[a, b] if 0 <= a <= 2 else jnp.zeros((chans, chans), BF16)
                    wp[w, at : at + chans, t * chans : (t + 1) * chans] = tap

    def load_backward(w, w_ref):
        for j in range(4):
            for b in range(3):
                at = (j * 3 + b) * chans
                for t in range(2):
                    a = j - t
                    if 0 <= a <= 2:
                        tap = w_ref[2 - a, 2 - b].astype(F32).T.astype(BF16)
                    else:
                        tap = jnp.zeros((chans, chans), BF16)
                    wp[w, at : at + chans, t * chans : (t + 1) * chans] = tap

    pairs = slots // 4

    def convolve(buf, w, out):
        def step(q, carry):
            base = q * (2 * pairs)
            pieces = []
            for p in range(pairs):
                pieces.append(
                    jnp.concatenate([buf[base + (2 * p + j)] for j in range(4)], axis=1)
                )
            result = jnp.dot(
                jnp.concatenate(pieces, axis=0), wp[w], preferred_element_type=F32
            )
            for p in range(pairs):
                for t in range(2):
                    out[base + (2 * p + t)] = result[
                        p * cols : (p + 1) * cols, t * chans : (t + 1) * chans
                    ]
            return carry

        lax.fori_loop(0, slots // (2 * pairs), step, 0)

    def kernel_grad(buf):
        acc[...] = jnp.zeros_like(acc)
        rows = 8

        def step(q, carry):
            base = q * rows + 1
            left = jnp.concatenate(
                [
                    jnp.concatenate([gt[base + (k + 2 - a)] for k in range(rows)], axis=1)
                    for a in range(3)
                ],
                axis=0,
            )
            right = jnp.concatenate([buf[base + k] for k in range(rows)], axis=0)
            acc[...] += jnp.dot(left, right, preferred_element_type=F32)
            return carry

        lax.fori_loop(0, slots // rows, step, 0)

    def edge_grads(top, bottom, turned):
        acc[0:chans] += jnp.dot(gt[2], top, preferred_element_type=F32)
        acc[2 * chans :] += jnp.dot(turned, bottom, preferred_element_type=F32)
        for a in range(3):
            for b in range(3):
                at = (a * 3 + b) * chans
                full[at : at + chans] = acc[
                    a * chans : (a + 1) * chans, b * chans : (b + 1) * chans
                ].T

    def scatter_images(k):
        for i in range(m):
            rs[k, i] = full[i * rows_out : (i + 1) * rows_out].astype(BF16)
        copies = []
        for d in range(1, m):
            peer = lax.rem(img + d, m)
            copy = pltpu.make_async_remote_copy(
                src_ref=rs.at[k, peer],
                dst_ref=got.at[k, d - 1],
                send_sem=s1_send.at[k, d - 1],
                recv_sem=s1_recv.at[k, d - 1],
                device_id={"img": peer},
                device_id_type=MESH,
            )
            copy.start()
            copies.append(copy)
        return copies

    def share_strips(k, before):
        wait_all(before)
        total = rs[k, img].astype(F32)
        for d in range(m - 1):
            total = total + got[k, d].astype(F32)
        ag[k, me] = total.astype(BF16)
        copies = []
        for d in range(1, n):
            copy = pltpu.make_async_remote_copy(
                src_ref=ag.at[k, me],
                dst_ref=ag.at[k, me],
                send_sem=s2_send.at[k, d - 1],
                recv_sem=s2_recv.at[k, d - 1],
                device_id={"strip": lax.rem(me + d, n)},
                device_id_type=MESH,
            )
            copy.start()
            copies.append(copy)
        return copies

    def finish_grad(k, before, target):
        wait_all(before)
        total = ag[k, 0].astype(F32)
        for s in range(1, n):
            total = total + ag[k, s].astype(F32)
        target[...] = total

    edge[0] = x_ref[0, last]
    edge[1] = g_ref[0, last]
    block = local_stats(lambda r: x_ref[0, r].astype(F32))
    build(bufd, lambda r: jnp.where(live(r), g_ref[0, r].astype(F32), 0.0))
    load_backward(1, w2_ref)
    pl.semaphore_wait(barrier, n - 1 + m - 1)
    stats1 = send_block(0, block)
    halo_x = send_halo(0, x_ref.at[0, 0], edge.at[0])
    halo_g = send_halo(1, g_ref.at[0, 0], edge.at[1])

    convolve(bufd, 1, back)
    load_forward(0, w1_ref)
    halo_x()
    wait_all(stats1)

    gain1, shift1 = gain1_ref[...], shift1_ref[...]
    gain2, shift2 = gain2_ref[...], shift2_ref[...]
    mean1, inv1 = joined_stats(0)

    def act_one(v):
        pre = (v - mean1) * inv1 * gain1 + shift1
        return pre * sigmoid(pre)

    build_joined(buf1, 0, lambda r: x_ref[0, r], act_one)
    convolve(buf1, 0, hidden)
    stats2 = send_block(1, local_stats(lambda r: hidden[r]))

    for k in (0, 1, slots + 2, slots + 3):
        gt[k] = jnp.zeros((chans, cols), BF16)

    def turn_cotangent(r, carry):
        gt[r + 2] = jnp.where(live(r), g_ref[0, r].astype(F32), 0.0).T.astype(BF16)
        return carry

    lax.fori_loop(0, slots, turn_cotangent, 0, unroll=4)
    load_backward(2, w1_ref)
    halo_g()
    edge_terms(1, 1)
    wait_all(stats2)
    mean2, inv2 = joined_stats(1)

    def slope_two(r, carry):
        sum_plain, sum_cross = carry
        normed = (hidden[r] - mean2) * inv2
        pre = normed * gain2 + shift2
        logistic = sigmoid(pre)
        act2[r] = (pre * logistic).astype(BF16)
        slope = logistic * (1.0 + pre * (1.0 - logistic))
        dpre = jnp.where(live(r), with_edges(r) * slope, 0.0)
        back[r] = dpre
        return sum_plain + fold(dpre), sum_cross + fold(dpre * normed)

    sum_plain, sum_cross = lax.fori_loop(0, slots, slope_two, (zero8, zero8))
    edge[2] = act2[last]
    sums2 = send_block(2, by_row([flat(sum_plain), flat(sum_cross)]))
    halo_a = send_halo(2, act2.at[0], edge.at[2])
    build(buf2, lambda r: jnp.where(live(r), act2[r].astype(F32), 0.0))
    kernel_grad(buf2)
    halo_a()
    top, bottom = arrived(2)
    edge_grads(top, bottom, gt[last + 2])
    wait_all(sums2)
    stage_two = scatter_images(1)
    total2 = joined_sums(2)
    mean_plain2, mean_cross2 = means_of(total2, gain2)

    def hidden_grad(r, carry):
        normed = (hidden[r] - mean2) * inv2
        value = inv2 * (back[r] * gain2 - mean_plain2 - normed * mean_cross2)
        value = jnp.where(live(r), value, 0.0)
        dh[r] = value.astype(BF16)
        gt[r + 2] = value.T.astype(BF16)
        return carry

    lax.fori_loop(0, slots, hidden_grad, 0, unroll=2)
    edge[3] = dh[last]
    halo_d = send_halo(3, dh.at[0], edge.at[3])
    kernel_grad(buf1)
    edge_grads(buf1[0], buf1[slots + 1], gt[slots + 1])
    stage_one = scatter_images(0)
    stage_two = share_strips(1, stage_two)
    build(bufd, lambda r: dh[r].astype(F32))
    convolve(bufd, 2, back)
    halo_d()
    edge_terms(3, 2)

    def slope_one(r, carry):
        sum_plain, sum_cross = carry
        normed = (x_ref[0, r].astype(F32) - mean1) * inv1
        pre = normed * gain1 + shift1
        logistic = sigmoid(pre)
        slope = logistic * (1.0 + pre * (1.0 - logistic))
        dpre = jnp.where(live(r), with_edges(r) * slope, 0.0)
        back[r] = dpre
        return sum_plain + fold(dpre), sum_cross + fold(dpre * normed)

    sum_plain, sum_cross = lax.fori_loop(0, slots, slope_one, (zero8, zero8))
    sums1 = send_block(3, by_row([flat(sum_plain), flat(sum_cross)]))
    stage_one = share_strips(0, stage_one)
    finish_grad(1, stage_two, grad2_ref)
    wait_all(sums1)
    total1 = joined_sums(3)
    mean_plain1, mean_cross1 = means_of(total1, gain1)

    def spread8(row):
        return jnp.broadcast_to(row, (8, chans))

    nbuf[img] = by_row(
        [spread8(total1[1:2]), spread8(total1[0:1]), spread8(total2[1:2]), spread8(total2[0:1])]
    )
    norms = []
    for d in range(1, m):
        copy = pltpu.make_async_remote_copy(
            src_ref=nbuf.at[img],
            dst_ref=nbuf.at[img],
            send_sem=n_send.at[d - 1],
            recv_sem=n_recv.at[d - 1],
            device_id={"img": lax.rem(img + d, m)},
            device_id_type=MESH,
        )
        copy.start()
        norms.append(copy)

    def image_grad(r, carry):
        normed = (x_ref[0, r].astype(F32) - mean1) * inv1
        branch = inv1 * (back[r] * gain1 - mean_plain1 - normed * mean_cross1)
        value = g_ref[0, r].astype(F32) + branch
        out_ref[0, r] = jnp.where(live(r), value, 0.0).astype(BF16)
        return carry

    lax.fori_loop(0, slots, image_grad, 0, unroll=2)
    wait_all(norms)
    total = nbuf[0]
    for i in range(1, m):
        total = total + nbuf[i]
    norm_ref[...] = total[0:4]
    finish_grad(0, stage_one, grad1_ref)


def body(
    image_in,
    cotangent,
    conv1_w,
    conv2_w,
    norm1_gain,
    norm1_shift,
    norm2_gain,
    norm2_shift,
    strip_rows,
):
    n = lax.axis_size("strip")
    m = lax.axis_size("img")
    _, slots, cols, chans = image_in.shape
    rows_out = 9 * chans // m
    vmem = pl.BlockSpec(memory_space=pltpu.VMEM)
    padded = slots + 2
    scratch = [
        pltpu.VMEM((padded, cols, 3 * chans), BF16),
        pltpu.VMEM((padded, cols, 3 * chans), BF16),
        pltpu.VMEM((padded, cols, 3 * chans), BF16),
        pltpu.VMEM((slots, cols, chans), F32),
        pltpu.VMEM((slots, cols, chans), F32),
        pltpu.VMEM((slots, cols, chans), BF16),
        pltpu.VMEM((slots, cols, chans), BF16),
        pltpu.VMEM((slots + 4, chans, cols), BF16),
        pltpu.VMEM((3, 12 * chans, 2 * chans), BF16),
        pltpu.VMEM((3 * chans, 3 * chans), F32),
        pltpu.VMEM((9 * chans, chans), F32),
        pltpu.VMEM((4, cols, chans), BF16),
        pltpu.VMEM((4, 2, cols, chans), BF16),
        pltpu.VMEM((4, n, 8, chans), F32),
        pltpu.VMEM((m, 8, chans), F32),
        pltpu.VMEM((2, m, rows_out, chans), BF16),
        pltpu.VMEM((2, m - 1, rows_out, chans), BF16),
        pltpu.VMEM((2, n, rows_out, chans), BF16),
        pltpu.VMEM((2, cols, chans), F32),
        pltpu.SemaphoreType.DMA((4, 2)),
        pltpu.SemaphoreType.DMA((4, 2)),
        pltpu.SemaphoreType.DMA((4, n - 1)),
        pltpu.SemaphoreType.DMA((4, n - 1)),
        pltpu.SemaphoreType.DMA((m - 1,)),
        pltpu.SemaphoreType.DMA((m - 1,)),
        pltpu.SemaphoreType.DMA((2, m - 1)),
        pltpu.SemaphoreType.DMA((2, m - 1)),
        pltpu.SemaphoreType.DMA((2, n - 1)),
        pltpu.SemaphoreType.DMA((2, n - 1)),
    ]
    return pl.pallas_call(
        functools.partial(kernel, n, m, rows_out),
        out_shape=(
            jax.ShapeDtypeStruct(image_in.shape, BF16),
            jax.ShapeDtypeStruct((rows_out, chans), F32),
            jax.ShapeDtypeStruct((rows_out, chans), F32),
            jax.ShapeDtypeStruct((4, chans), F32),
        ),
        in_specs=[pl.BlockSpec(memory_space=pltpu.SMEM)] + [vmem] * 8,
        out_specs=(vmem,) * 4,
        scratch_shapes=scratch,
        compiler_params=pltpu.CompilerParams(
            collective_id=0, has_side_effects=True, vmem_limit_bytes=32 * 1024 * 1024
        ),
    )(
        strip_rows,
        image_in,
        cotangent,
        conv1_w,
        conv2_w,
        norm1_gain.reshape(1, chans),
        norm1_shift.reshape(1, chans),
        norm2_gain.reshape(1, chans),
        norm2_shift.reshape(1, chans),
    )


def solution(mesh):
    placed = (
        P("img", "strip", None, None),
        P("img", "strip", None, None),
        P(),
        P(),
        P(),
        P(),
        P(),
        P(),
        P("img", "strip"),
    )
    return jax.shard_map(
        body,
        mesh=mesh,
        in_specs=placed,
        out_specs=(P("img", "strip", None, None), P("img", None), P("img", None), P()),
        check_vma=False,
    )
```

```python
import functools

import jax
import jax.numpy as jnp
from jax import lax
from jax.experimental import pallas as pl
from jax.experimental.pallas import tpu as pltpu
from jax.sharding import PartitionSpec as P

GROUPS = 32
EPSILON = 1e-06
F32 = jnp.float32
BF16 = jnp.bfloat16
CHUNKS = 4
MESH = pl.DeviceIdType.MESH


def sigmoid(z):
    return 0.5 * jnp.tanh(0.5 * z) + 0.5


def group_sum(block, size):
    lanes = block.shape[1]
    lane = lax.broadcasted_iota(jnp.int32, block.shape, 1)
    step = 1
    while step < size:
        upper = pltpu.roll(block, lanes - step, 1)
        lower = pltpu.roll(block, step, 1)
        block = block + jnp.where((lane & step) == 0, upper, lower)
        step *= 2
    return block


def fold(values):
    return jnp.sum(values.reshape(values.shape[0] // 8, 8, values.shape[1]), axis=0)


def flat(block):
    return jnp.broadcast_to(jnp.sum(block, axis=0, keepdims=True), block.shape)


def by_row(parts):
    row = lax.broadcasted_iota(jnp.int32, parts[0].shape, 0)
    out = jnp.zeros_like(parts[0])
    for k, part in enumerate(parts):
        out = jnp.where(row == k, part, out)
    return out


def kernel(
    n,
    m,
    rows_out,
    len_ref,
    x_hbm,
    g_hbm,
    w1_hbm,
    w2_hbm,
    gain1_hbm,
    shift1_hbm,
    gain2_hbm,
    shift2_hbm,
    out_ref,
    grad1_ref,
    grad2_ref,
    norm_ref,
    x_ref,
    g_ref,
    w1_ref,
    w2_ref,
    params,
    load_sem,
    buf1,
    buf2,
    bufd,
    hidden,
    back,
    act2,
    dh,
    gt,
    wp,
    acc,
    full,
    edge,
    halo,
    xbuf,
    nbuf,
    rs,
    got,
    ag,
    corr,
    halo_send,
    halo_recv,
    x_send,
    x_recv,
    n_send,
    n_recv,
    s1_send,
    s1_recv,
    s2_send,
    s2_recv,
):
    _, slots, cols, chans = x_ref.shape
    size = chans // GROUPS
    me = lax.axis_index("strip")
    img = lax.axis_index("img")
    length = len_ref[0, 0]
    last = jnp.maximum(length - 1, 0)
    height = slots * n // 2
    cells = float(height * cols * size)

    barrier = pltpu.get_barrier_semaphore()
    for d in range(1, n):
        pl.semaphore_signal(
            barrier, inc=1, device_id={"strip": lax.rem(me + d, n)}, device_id_type=MESH
        )
    for d in range(1, m):
        pl.semaphore_signal(
            barrier, inc=1, device_id={"img": lax.rem(img + d, m)}, device_id_type=MESH
        )

    piece = slots // CHUNKS
    loads = [
        pltpu.make_async_copy(
            x_hbm.at[0, pl.ds(c * piece, piece)],
            x_ref.at[0, pl.ds(c * piece, piece)],
            load_sem.at[c],
        )
        for c in range(CHUNKS)
    ]
    for k, (source, target) in enumerate(((g_hbm, g_ref), (w2_hbm, w2_ref), (w1_hbm, w1_ref))):
        loads.append(pltpu.make_async_copy(source, target, load_sem.at[CHUNKS + k]))
    for k, source in enumerate((gain1_hbm, shift1_hbm, gain2_hbm, shift2_hbm)):
        loads.append(pltpu.make_async_copy(source, params.at[k], load_sem.at[CHUNKS + 3 + k]))
    for load in loads:
        load.start()

    def send_halo(kind, first, last):
        below = pltpu.make_async_remote_copy(
            src_ref=last,
            dst_ref=halo.at[kind, 0],
            send_sem=halo_send.at[kind, 0],
            recv_sem=halo_recv.at[kind, 0],
            device_id={"strip": lax.rem(me + 1, n)},
            device_id_type=MESH,
        )
        above = pltpu.make_async_remote_copy(
            src_ref=first,
            dst_ref=halo.at[kind, 1],
            send_sem=halo_send.at[kind, 1],
            recv_sem=halo_recv.at[kind, 1],
            device_id={"strip": lax.rem(me + n - 1, n)},
            device_id_type=MESH,
        )
        pl.when(me < n - 1)(below.start)
        pl.when(me > 0)(above.start)

        def wait():
            @pl.when(me < n - 1)
            def _():
                below.wait_send()
                above.wait_recv()

            @pl.when(me > 0)
            def _():
                above.wait_send()
                below.wait_recv()

        return wait

    def send_block(kind, block):
        xbuf[kind, me] = block
        copies = []
        for d in range(1, n):
            copy = pltpu.make_async_remote_copy(
                src_ref=xbuf.at[kind, me],
                dst_ref=xbuf.at[kind, me],
                send_sem=x_send.at[kind, d - 1],
                recv_sem=x_recv.at[kind, d - 1],
                device_id={"strip": lax.rem(me + d, n)},
                device_id_type=MESH,
            )
            copy.start()
            copies.append(copy)
        return copies

    def wait_all(copies):
        for copy in copies:
            copy.wait()

    def live(row):
        return jnp.full((cols, chans), row, jnp.int32) < length

    zero8 = jnp.zeros((8, chans), F32)

    def add_rows(load, start, count, total):
        def add(r, total):
            return total + fold(jnp.where(live(r), load(r), 0.0))

        return lax.fori_loop(start, start + count, add, total, unroll=2)

    def local_stats(load, total):
        count = (jnp.full((8, chans), length, jnp.int32) * (cols * size)).astype(F32)
        mean = group_sum(flat(total), size) / count
        one = mean[0:1]

        def spread(r, total):
            centered = jnp.where(live(r), load(r) - one, 0.0)
            return total + fold(centered * centered)

        spread_sum = lax.fori_loop(0, slots, spread, zero8, unroll=2)
        return by_row([count, mean, group_sum(flat(spread_sum), size)])

    def joined_stats(kind):
        count = xbuf[kind, 0, 0:1]
        weighted = count * xbuf[kind, 0, 1:2]
        total = count
        for k in range(1, n):
            count = xbuf[kind, k, 0:1]
            total = total + count
            weighted = weighted + count * xbuf[kind, k, 1:2]
        mean = weighted / total
        spread = jnp.zeros_like(mean)
        for k in range(n):
            delta = xbuf[kind, k, 1:2] - mean
            spread = spread + (xbuf[kind, k, 2:3] + xbuf[kind, k, 0:1] * delta * delta)
        return mean, lax.rsqrt(spread / cells + EPSILON)

    def joined_sums(kind):
        total = xbuf[kind, 0]
        for k in range(1, n):
            total = total + xbuf[kind, k]
        return total

    def means_of(sums, gain):
        both = group_sum(sums * gain, size) / cells
        return both[0:1], both[1:2]

    column = lax.broadcasted_iota(jnp.int32, (cols, chans), 0)
    has_above = jnp.where(me > 0, 1, 0)
    has_below = jnp.where(me < n - 1, 1, 0)

    def shifted(value):
        before = jnp.where(column == 0, 0.0, pltpu.roll(value, 1, 0))
        after = jnp.where(column == cols - 1, 0.0, pltpu.roll(value, cols - 1, 0))
        return before.astype(BF16), value.astype(BF16), after.astype(BF16)

    def put(buf, i, value):
        for b, piece in enumerate(shifted(value)):
            buf[i, :, b * chans : (b + 1) * chans] = piece

    def clear(buf, i):
        buf[i] = jnp.zeros((cols, 3 * chans), BF16)

    def build(buf, load):
        def one_row(r, carry):
            put(buf, r + 1, load(r))
            return carry

        lax.fori_loop(0, slots, one_row, 0, unroll=2)
        clear(buf, 0)
        clear(buf, slots + 1)

    def build_joined(buf, kind, load, change):
        def one_row(i, carry):
            r = i - 1
            own = load(jnp.clip(r, 0, slots - 1)).astype(F32)
            at = jnp.full((cols, chans), r, jnp.int32)
            value = jnp.where(at < 0, halo[kind, 0].astype(F32), own)
            value = jnp.where(at == length, halo[kind, 1].astype(F32), value)
            keep = jnp.where(at < 0, has_above, jnp.where(at == length, has_below, 1))
            keep = jnp.where(at > length, 0, keep)
            put(buf, i, jnp.where(keep > 0, change(value), 0.0))
            return carry

        lax.fori_loop(0, slots + 2, one_row, 0, unroll=2)

    def arrived(kind):
        flags = (has_above, has_below)
        return [
            jnp.concatenate(
                shifted(
                    jnp.where(
                        jnp.full((cols, chans), flags[e], jnp.int32) > 0,
                        halo[kind, e].astype(F32),
                        0.0,
                    )
                ),
                axis=1,
            )
            for e in range(2)
        ]

    def edge_terms(kind, w):
        top, bottom = arrived(kind)
        taps = 3 * chans
        corr[0] = jnp.dot(top, wp[w, 0:taps, 0:chans], preferred_element_type=F32)
        corr[1] = jnp.dot(bottom, wp[w, 2 * taps : 3 * taps, 0:chans], preferred_element_type=F32)

    def with_edges(r):
        at = jnp.full((cols, chans), r, jnp.int32)
        value = back[r] + jnp.where(at == 0, corr[0], 0.0)
        return value + jnp.where(at == last, corr[1], 0.0)

    def load_forward(w, w_ref):
        for j in range(4):
            for b in range(3):
                at = (j * 3 + b) * chans
                for t in range(2):
                    a = j - t
                    tap = w_ref[a, b] if 0 <= a <= 2 else jnp.zeros((chans, chans), BF16)
                    wp[w, at : at + chans, t * chans : (t + 1) * chans] = tap

    def load_backward(w, w_ref):
        for j in range(4):
            for b in range(3):
                at = (j * 3 + b) * chans
                for t in range(2):
                    a = j - t
                    if 0 <= a <= 2:
                        tap = w_ref[2 - a, 2 - b].astype(F32).T.astype(BF16)
                    else:
                        tap = jnp.zeros((chans, chans), BF16)
                    wp[w, at : at + chans, t * chans : (t + 1) * chans] = tap

    pairs = slots // 4

    def convolve(buf, w, out, summed=False):
        def step(q, carry):
            base = q * (2 * pairs)
            pieces = []
            for p in range(pairs):
                pieces.append(
                    jnp.concatenate([buf[base + (2 * p + j)] for j in range(4)], axis=1)
                )
            result = jnp.dot(
                jnp.concatenate(pieces, axis=0), wp[w], preferred_element_type=F32
            )
            for p in range(pairs):
                for t in range(2):
                    row = base + (2 * p + t)
                    value = result[p * cols : (p + 1) * cols, t * chans : (t + 1) * chans]
                    out[row] = value
                    if summed:
                        carry = carry + fold(jnp.where(live(row), value, 0.0))
            return carry

        return lax.fori_loop(0, slots // (2 * pairs), step, zero8)

    def kernel_grad(buf):
        acc[...] = jnp.zeros_like(acc)
        rows = 8

        def step(q, carry):
            base = q * rows + 1
            left = jnp.concatenate(
                [
                    jnp.concatenate([gt[base + (k + 2 - a)] for k in range(rows)], axis=1)
                    for a in range(3)
                ],
                axis=0,
            )
            right = jnp.concatenate([buf[base + k] for k in range(rows)], axis=0)
            acc[...] += jnp.dot(left, right, preferred_element_type=F32)
            return carry

        lax.fori_loop(0, slots // rows, step, 0)

    def edge_grads(top, bottom, turned):
        acc[0:chans] += jnp.dot(gt[2], top, preferred_element_type=F32)
        acc[2 * chans :] += jnp.dot(turned, bottom, preferred_element_type=F32)
        for a in range(3):
            for b in range(3):
                at = (a * 3 + b) * chans
                full[at : at + chans] = acc[
                    a * chans : (a + 1) * chans, b * chans : (b + 1) * chans
                ].T

    def scatter_images(k):
        for i in range(m):
            rs[k, i] = full[i * rows_out : (i + 1) * rows_out].astype(BF16)
        copies = []
        for d in range(1, m):
            peer = lax.rem(img + d, m)
            copy = pltpu.make_async_remote_copy(
                src_ref=rs.at[k, peer],
                dst_ref=got.at[k, d - 1],
                send_sem=s1_send.at[k, d - 1],
                recv_sem=s1_recv.at[k, d - 1],
                device_id={"img": peer},
                device_id_type=MESH,
            )
            copy.start()
            copies.append(copy)
        return copies

    def share_strips(k, before):
        wait_all(before)
        total = rs[k, img].astype(F32)
        for d in range(m - 1):
            total = total + got[k, d].astype(F32)
        ag[k, me] = total.astype(BF16)
        copies = []
        for d in range(1, n):
            copy = pltpu.make_async_remote_copy(
                src_ref=ag.at[k, me],
                dst_ref=ag.at[k, me],
                send_sem=s2_send.at[k, d - 1],
                recv_sem=s2_recv.at[k, d - 1],
                device_id={"strip": lax.rem(me + d, n)},
                device_id_type=MESH,
            )
            copy.start()
            copies.append(copy)
        return copies

    def finish_grad(k, before, target):
        wait_all(before)
        total = ag[k, 0].astype(F32)
        for s in range(1, n):
            total = total + ag[k, s].astype(F32)
        target[...] = total

    def source(r):
        return x_ref[0, r].astype(F32)

    total = zero8
    for c in range(CHUNKS):
        loads[c].wait()
        total = add_rows(source, c * piece, piece, total)
    edge[0] = x_ref[0, last]
    block = local_stats(source, total)
    loads[CHUNKS].wait()
    edge[1] = g_ref[0, last]
    build(bufd, lambda r: jnp.where(live(r), g_ref[0, r].astype(F32), 0.0))
    loads[CHUNKS + 1].wait()
    load_backward(1, w2_ref)
    pl.semaphore_wait(barrier, n - 1 + m - 1)
    stats1 = send_block(0, block)
    halo_x = send_halo(0, x_ref.at[0, 0], edge.at[0])
    halo_g = send_halo(1, g_ref.at[0, 0], edge.at[1])

    convolve(bufd, 1, back)
    loads[CHUNKS + 2].wait()
    load_forward(0, w1_ref)
    halo_x()
    wait_all(stats1)

    for k in range(4):
        loads[CHUNKS + 3 + k].wait()
    gain1, shift1, gain2, shift2 = params[0], params[1], params[2], params[3]
    mean1, inv1 = joined_stats(0)

    def act_one(v):
        pre = (v - mean1) * inv1 * gain1 + shift1
        return pre * sigmoid(pre)

    build_joined(buf1, 0, lambda r: x_ref[0, r], act_one)
    total = convolve(buf1, 0, hidden, summed=True)
    stats2 = send_block(1, local_stats(lambda r: hidden[r], total))

    for k in (0, 1, slots + 2, slots + 3):
        gt[k] = jnp.zeros((chans, cols), BF16)

    def turn_cotangent(r, carry):
        gt[r + 2] = jnp.where(live(r), g_ref[0, r].astype(F32), 0.0).T.astype(BF16)
        return carry

    lax.fori_loop(0, slots, turn_cotangent, 0, unroll=4)
    load_backward(2, w1_ref)
    halo_g()
    edge_terms(1, 1)
    wait_all(stats2)
    mean2, inv2 = joined_stats(1)

    def slope_two(r, carry):
        sum_plain, sum_cross = carry
        normed = (hidden[r] - mean2) * inv2
        pre = normed * gain2 + shift2
        logistic = sigmoid(pre)
        act2[r] = (pre * logistic).astype(BF16)
        slope = logistic * (1.0 + pre * (1.0 - logistic))
        dpre = jnp.where(live(r), with_edges(r) * slope, 0.0)
        back[r] = dpre
        return sum_plain + fold(dpre), sum_cross + fold(dpre * normed)

    sum_plain, sum_cross = lax.fori_loop(0, slots, slope_two, (zero8, zero8), unroll=2)
    edge[2] = act2[last]
    sums2 = send_block(2, by_row([flat(sum_plain), flat(sum_cross)]))
    halo_a = send_halo(2, act2.at[0], edge.at[2])
    build(buf2, lambda r: jnp.where(live(r), act2[r].astype(F32), 0.0))
    kernel_grad(buf2)
    halo_a()
    top, bottom = arrived(2)
    edge_grads(top, bottom, gt[last + 2])
    wait_all(sums2)
    stage_two = scatter_images(1)
    total2 = joined_sums(2)
    mean_plain2, mean_cross2 = means_of(total2, gain2)

    def hidden_grad(r, carry):
        normed = (hidden[r] - mean2) * inv2
        value = inv2 * (back[r] * gain2 - mean_plain2 - normed * mean_cross2)
        value = jnp.where(live(r), value, 0.0)
        dh[r] = value.astype(BF16)
        gt[r + 2] = value.T.astype(BF16)
        return carry

    lax.fori_loop(0, slots, hidden_grad, 0, unroll=2)
    edge[3] = dh[last]
    halo_d = send_halo(3, dh.at[0], edge.at[3])
    kernel_grad(buf1)
    edge_grads(buf1[0], buf1[slots + 1], gt[slots + 1])
    stage_one = scatter_images(0)
    build(bufd, lambda r: dh[r].astype(F32))
    stage_two = share_strips(1, stage_two)
    convolve(bufd, 2, back)
    halo_d()
    edge_terms(3, 2)

    def slope_one(r, carry):
        sum_plain, sum_cross = carry
        normed = (x_ref[0, r].astype(F32) - mean1) * inv1
        pre = normed * gain1 + shift1
        logistic = sigmoid(pre)
        slope = logistic * (1.0 + pre * (1.0 - logistic))
        dpre = jnp.where(live(r), with_edges(r) * slope, 0.0)
        back[r] = dpre
        return sum_plain + fold(dpre), sum_cross + fold(dpre * normed)

    sum_plain, sum_cross = lax.fori_loop(0, slots, slope_one, (zero8, zero8), unroll=2)
    sums1 = send_block(3, by_row([flat(sum_plain), flat(sum_cross)]))
    stage_one = share_strips(0, stage_one)
    finish_grad(1, stage_two, grad2_ref)
    wait_all(sums1)
    total1 = joined_sums(3)
    mean_plain1, mean_cross1 = means_of(total1, gain1)

    def spread8(row):
        return jnp.broadcast_to(row, (8, chans))

    nbuf[img] = by_row(
        [spread8(total1[1:2]), spread8(total1[0:1]), spread8(total2[1:2]), spread8(total2[0:1])]
    )
    norms = []
    for d in range(1, m):
        copy = pltpu.make_async_remote_copy(
            src_ref=nbuf.at[img],
            dst_ref=nbuf.at[img],
            send_sem=n_send.at[d - 1],
            recv_sem=n_recv.at[d - 1],
            device_id={"img": lax.rem(img + d, m)},
            device_id_type=MESH,
        )
        copy.start()
        norms.append(copy)

    def image_grad(r, carry):
        normed = (x_ref[0, r].astype(F32) - mean1) * inv1
        branch = inv1 * (back[r] * gain1 - mean_plain1 - normed * mean_cross1)
        value = g_ref[0, r].astype(F32) + branch
        out_ref[0, r] = jnp.where(live(r), value, 0.0).astype(BF16)
        return carry

    lax.fori_loop(0, slots, image_grad, 0, unroll=2)
    wait_all(norms)
    total = nbuf[0]
    for i in range(1, m):
        total = total + nbuf[i]
    norm_ref[...] = total[0:4]
    finish_grad(0, stage_one, grad1_ref)


def place(*refs):
    sems = refs[-1]
    copies = [pltpu.make_async_copy(refs[k], refs[4 + k], sems.at[k]) for k in range(4)]
    for copy in copies:
        copy.start()
    for copy in copies:
        copy.wait()


def body(
    image_in,
    cotangent,
    conv1_w,
    conv2_w,
    norm1_gain,
    norm1_shift,
    norm2_gain,
    norm2_shift,
    strip_rows,
):
    n = lax.axis_size("strip")
    m = lax.axis_size("img")
    _, slots, cols, chans = image_in.shape
    rows_out = 9 * chans // m
    vmem = pl.BlockSpec(memory_space=pltpu.VMEM)
    hbm = pl.BlockSpec(memory_space=pltpu.HBM)
    padded = slots + 2
    scratch = [
        pltpu.VMEM(image_in.shape, BF16),
        pltpu.VMEM(cotangent.shape, BF16),
        pltpu.VMEM(conv1_w.shape, BF16),
        pltpu.VMEM(conv2_w.shape, BF16),
        pltpu.VMEM((4, 1, chans), F32),
        pltpu.SemaphoreType.DMA((CHUNKS + 7,)),
        pltpu.VMEM((padded, cols, 3 * chans), BF16),
        pltpu.VMEM((padded, cols, 3 * chans), BF16),
        pltpu.VMEM((padded, cols, 3 * chans), BF16),
        pltpu.VMEM((slots, cols, chans), F32),
        pltpu.VMEM((slots, cols, chans), F32),
        pltpu.VMEM((slots, cols, chans), BF16),
        pltpu.VMEM((slots, cols, chans), BF16),
        pltpu.VMEM((slots + 4, chans, cols), BF16),
        pltpu.VMEM((3, 12 * chans, 2 * chans), BF16),
        pltpu.VMEM((3 * chans, 3 * chans), F32),
        pltpu.VMEM((9 * chans, chans), F32),
        pltpu.VMEM((4, cols, chans), BF16),
        pltpu.VMEM((4, 2, cols, chans), BF16),
        pltpu.VMEM((4, n, 8, chans), F32),
        pltpu.VMEM((m, 8, chans), F32),
        pltpu.VMEM((2, m, rows_out, chans), BF16),
        pltpu.VMEM((2, m - 1, rows_out, chans), BF16),
        pltpu.VMEM((2, n, rows_out, chans), BF16),
        pltpu.VMEM((2, cols, chans), F32),
        pltpu.SemaphoreType.DMA((4, 2)),
        pltpu.SemaphoreType.DMA((4, 2)),
        pltpu.SemaphoreType.DMA((4, n - 1)),
        pltpu.SemaphoreType.DMA((4, n - 1)),
        pltpu.SemaphoreType.DMA((m - 1,)),
        pltpu.SemaphoreType.DMA((m - 1,)),
        pltpu.SemaphoreType.DMA((2, m - 1)),
        pltpu.SemaphoreType.DMA((2, m - 1)),
        pltpu.SemaphoreType.DMA((2, n - 1)),
        pltpu.SemaphoreType.DMA((2, n - 1)),
    ]
    results = pl.pallas_call(
        functools.partial(kernel, n, m, rows_out),
        out_shape=(
            jax.ShapeDtypeStruct(image_in.shape, BF16),
            jax.ShapeDtypeStruct((rows_out, chans), F32),
            jax.ShapeDtypeStruct((rows_out, chans), F32),
            jax.ShapeDtypeStruct((4, chans), F32),
        ),
        in_specs=[pl.BlockSpec(memory_space=pltpu.SMEM)] + [hbm] * 8,
        out_specs=(vmem,) * 4,
        scratch_shapes=scratch,
        compiler_params=pltpu.CompilerParams(
            collective_id=0, has_side_effects=True, vmem_limit_bytes=32 * 1024 * 1024
        ),
    )(
        strip_rows,
        pltpu.with_memory_space_constraint(image_in, pltpu.HBM),
        pltpu.with_memory_space_constraint(cotangent, pltpu.HBM),
        pltpu.with_memory_space_constraint(conv1_w, pltpu.HBM),
        pltpu.with_memory_space_constraint(conv2_w, pltpu.HBM),
        pltpu.with_memory_space_constraint(norm1_gain.reshape(1, chans), pltpu.HBM),
        pltpu.with_memory_space_constraint(norm1_shift.reshape(1, chans), pltpu.HBM),
        pltpu.with_memory_space_constraint(norm2_gain.reshape(1, chans), pltpu.HBM),
        pltpu.with_memory_space_constraint(norm2_shift.reshape(1, chans), pltpu.HBM),
    )
    return pl.pallas_call(
        place,
        out_shape=tuple(jax.ShapeDtypeStruct(r.shape, r.dtype) for r in results),
        in_specs=[vmem] * 4,
        out_specs=(hbm,) * 4,
        scratch_shapes=[pltpu.SemaphoreType.DMA((4,))],
        compiler_params=pltpu.CompilerParams(vmem_limit_bytes=4 * 1024 * 1024),
    )(*results)


def solution(mesh):
    placed = (
        P("img", "strip", None, None),
        P("img", "strip", None, None),
        P(),
        P(),
        P(),
        P(),
        P(),
        P(),
        P("img", "strip"),
    )
    return jax.shard_map(
        body,
        mesh=mesh,
        in_specs=placed,
        out_specs=(P("img", "strip", None, None), P("img", None), P("img", None), P()),
        check_vma=False,
    )
```
